32 devices in a mesh: views: 2 (over core), rows: 8 (over z, x), chan: 2 (over y).
Axes of the slice: x: 2, y: 2, z: 4, core: 2. Of those that a mesh axis runs over, the one named last changes fastest.
Arguments:
- latent: bfloat16 [32, 384, 256], P(('views', 'rows'), 'chan'), parts along dimension 0, may hold values from -6 to 6
- cache_low_a: bfloat16 [2, 32, 384, 256], P(None, ('views', 'rows'), 'chan'), parts along dimension 1, may hold values from -6 to 6
- cache_low_b: bfloat16 [2, 32, 384, 256], P(None, ('views', 'rows'), 'chan'), parts along dimension 1, may hold values from -6 to 6
- gain_low_a: bfloat16 [384], P('chan'), may hold values from 0.5 to 1.5
- gain_low_b: bfloat16 [384], P('chan'), may hold values from 0.5 to 1.5
- kernel_low_a: bfloat16 [3, 3, 3, 384, 384], P(None, None, None, 'chan'), may hold values from -0.0625 to 0.0625
- kernel_low_b: bfloat16 [3, 3, 3, 384, 384], P(None, None, None, 'chan'), may hold values from -0.0625 to 0.0625
- resample_kernel: bfloat16 [3, 3, 192, 384], P(None, None, 'rows'), may hold values from -0.109375 to 0.109375
- gain_high_a: bfloat16 [192], replicated, may hold values from 0.5 to 1.5
- gain_high_b: bfloat16 [192], replicated, may hold values from 0.5 to 1.5
- kernel_high_a: bfloat16 [3, 3, 3, 192, 192], P(None, None, None, 'rows'), may hold values from -0.078125 to 0.078125
- kernel_high_b: bfloat16 [3, 3, 3, 192, 192], P(None, None, None, 'rows'), may hold values from -0.078125 to 0.078125
- cache_high_a: bfloat16 [2, 64, 192, 512], P(None, ('views', 'rows'), None, 'chan'), parts along dimension 1, may hold values from -6 to 6
- cache_high_b: bfloat16 [2, 64, 192, 512], P(None, ('views', 'rows'), None, 'chan'), parts along dimension 1, may hold values from -6 to 6
Outputs:
- decoded: bfloat16 [64, 192, 512], P(('views', 'rows'), None, 'chan'), parts along dimension 0
The draws below stay inside these ranges and needn't reach their ends.
There are 2 independent parts, one for each index of `views`. The reference program is written for one: setup_inputs(seed, part) draws one part's arguments, and reference() takes and returns one part's arrays. A program takes and returns all parts, laid end to end along the dimension named above; an argument that names none is the same for every part. Nothing has to cross between parts.
All inputs are finite; a program needn't handle non-finite values.
Results may differ from the reference program's by a relative error of at most 0.0095.
Values may be sent and summed in bfloat16 or wider, within the bound.
No kernel may reach another device: no remote copies, remote signals or barrier semaphores. Data moves between devices by JAX's collectives and lax.ppermute only.
A program may use at most 128 MiB of HBM per device.

```python
import jax
import jax.numpy as jnp
from jax import lax

C1 = 384
C2 = 192
W1 = 256
H1 = 16
H2 = 32
W2 = 512


def block_levels(stream_key, dims, split, low, top_value):
    def one(dim, blocks):
        steps = jax.random.uniform(jax.random.fold_in(jax.random.fold_in(stream_key, 6), dim), (blocks,), jnp.float32, low / len(split), top_value / len(split))
        return jnp.repeat(jnp.exp(steps), dims[dim] // blocks).reshape((-1,) + (1,) * (len(dims) - dim - 1))

    factor_of = one(*split[0])
    for cut in split[1:]:
        factor_of = factor_of * one(*cut)
    return factor_of


def scatter_about(rng, extent, spread, limit, cuts=(), held_as=jnp.bfloat16):
    values = spread * jax.random.normal(rng, extent, jnp.float32)
    if cuts:
        values = values * block_levels(rng, extent, cuts, -0.22, 0.18)
    return jnp.clip(values, -limit, limit).astype(held_as)


def setup_inputs(seed: int = 0, part: int = 0) -> dict:
    arg_keys = jax.random.split(jax.random.key(seed), 15)
    part_splits = jax.random.split(jax.random.fold_in(arg_keys[14], part), 15)
    latent = scatter_about(part_splits[0], (H1, C1, W1), 1.0, 6.0, ((0, 8), (1, 2)))
    cache_low_a = scatter_about(part_splits[1], (2, H1, C1, W1), 1.0, 6.0, ((1, 8), (2, 2)))
    cache_low_b = scatter_about(part_splits[2], (2, H1, C1, W1), 1.0, 6.0, ((1, 8), (2, 2)))
    gain_low_a = jnp.clip(0.5 + 1.0 * jax.random.uniform(arg_keys[3], (C1,), jnp.float32) ** block_levels(arg_keys[3], (C1,), ((0, 2),), -0.2, 0.2), 0.5, 1.5).astype(jnp.bfloat16)
    gain_low_b = jnp.clip(0.5 + 1.0 * jax.random.uniform(arg_keys[4], (C1,), jnp.float32) ** block_levels(arg_keys[4], (C1,), ((0, 2),), -0.2, 0.2), 0.5, 1.5).astype(jnp.bfloat16)
    kernel_low_a = scatter_about(arg_keys[5], (3, 3, 3, C1, C1), (27 * C1) ** -0.5, 0.0625, ((3, 2),))
    kernel_low_b = scatter_about(arg_keys[6], (3, 3, 3, C1, C1), (27 * C1) ** -0.5, 0.0625, ((3, 2),))
    resample_kernel = scatter_about(arg_keys[7], (3, 3, C2, C1), (9 * C1) ** -0.5, 0.109375, ((2, 8),))
    gain_high_a = jnp.clip(jax.random.uniform(arg_keys[8], (C2,), jnp.float32, 0.5, 1.5), 0.5, 1.5).astype(jnp.bfloat16)
    gain_high_b = jnp.clip(jax.random.uniform(arg_keys[9], (C2,), jnp.float32, 0.5, 1.5), 0.5, 1.5).astype(jnp.bfloat16)
    kernel_high_a = scatter_about(arg_keys[10], (3, 3, 3, C2, C2), (27 * C2) ** -0.5, 0.078125, ((3, 8),))
    kernel_high_b = scatter_about(arg_keys[11], (3, 3, 3, C2, C2), (27 * C2) ** -0.5, 0.078125, ((3, 8),))
    cache_high_a = scatter_about(part_splits[12], (2, H2, C2, W2), 1.0, 6.0, ((1, 8), (3, 2)))
    cache_high_b = scatter_about(part_splits[13], (2, H2, C2, W2), 1.0, 6.0, ((1, 8), (3, 2)))
    return {"latent": latent, "cache_low_a": cache_low_a, "cache_low_b": cache_low_b, "gain_low_a": gain_low_a, "gain_low_b": gain_low_b, "kernel_low_a": kernel_low_a, "kernel_low_b": kernel_low_b, "resample_kernel": resample_kernel, "gain_high_a": gain_high_a, "gain_high_b": gain_high_b, "kernel_high_a": kernel_high_a, "kernel_high_b": kernel_high_b, "cache_high_a": cache_high_a, "cache_high_b": cache_high_b}


def norm_silu(inputs, gains):
    values = inputs.astype(jnp.float32)
    scaled = values * lax.rsqrt(lax.optimization_barrier(jnp.mean(values * values, axis=-1, keepdims=True)) + 1e-06) * gains.astype(jnp.float32)
    return (scaled * jax.nn.sigmoid(scaled)).astype(jnp.bfloat16)

def plane_conv(planes, kernel):
    return lax.conv_general_dilated(planes[None].astype(jnp.float32), kernel.astype(jnp.float32), (1, 1), ((1, 1), (1, 1)), dimension_numbers=('NHWC', 'HWIO', 'NHWC'), precision=lax.Precision.HIGHEST)[0]

def causal_conv(cached, living, kernel):
    frames = jnp.concatenate([cached, living[None]], axis=0)
    totals = plane_conv(frames[0], kernel[0])
    for offset in range(1, 3):
        totals = totals + plane_conv(frames[offset], kernel[offset])
    return totals

def reference(latent, cache_low_a, cache_low_b, gain_low_a, gain_low_b, kernel_low_a, kernel_low_b, resample_kernel, gain_high_a, gain_high_b, kernel_high_a, kernel_high_b, cache_high_a, cache_high_b):
    latent = jnp.transpose(latent, (0, 2, 1))
    cache_low_a = jnp.transpose(cache_low_a, (0, 1, 3, 2))
    cache_low_b = jnp.transpose(cache_low_b, (0, 1, 3, 2))
    cache_high_a = jnp.transpose(cache_high_a, (0, 1, 3, 2))
    cache_high_b = jnp.transpose(cache_high_b, (0, 1, 3, 2))
    kernel_low_a = jnp.transpose(kernel_low_a, (0, 1, 2, 4, 3))
    kernel_low_b = jnp.transpose(kernel_low_b, (0, 1, 2, 4, 3))
    kernel_high_a = jnp.transpose(kernel_high_a, (0, 1, 2, 4, 3))
    kernel_high_b = jnp.transpose(kernel_high_b, (0, 1, 2, 4, 3))
    resample_kernel = jnp.transpose(resample_kernel, (0, 1, 3, 2))
    middle_low = causal_conv(cache_low_a, norm_silu(latent, gain_low_a), kernel_low_a).astype(jnp.bfloat16)
    level_one = (latent.astype(jnp.float32) + causal_conv(cache_low_b, norm_silu(middle_low, gain_low_b), kernel_low_b)).astype(jnp.bfloat16)
    upsampled = jnp.repeat(jnp.repeat(level_one, 2, axis=0), 2, axis=1)
    resampled = plane_conv(upsampled, resample_kernel).astype(jnp.bfloat16)
    middle_high = causal_conv(cache_high_a, norm_silu(resampled, gain_high_a), kernel_high_a).astype(jnp.bfloat16)
    decoded = (resampled.astype(jnp.float32) + causal_conv(cache_high_b, norm_silu(middle_high, gain_high_b), kernel_high_b)).astype(jnp.bfloat16)
    return jnp.transpose(decoded, (0, 2, 1))
```

```python
import functools

import jax
import jax.numpy as jnp
from jax import lax
from jax.experimental import pallas as pl
from jax.experimental.pallas import tpu as pltpu
from jax.sharding import PartitionSpec as P

F32, BF16 = jnp.float32, jnp.bfloat16
GRANT = 56 * 1024 * 1024


def in_vmem(*shape):
    return pl.BlockSpec(shape, lambda *_: (0,) * len(shape))


SCALAR = pl.BlockSpec(memory_space=pltpu.SMEM)


def call(body, name, args, specs, outs, scratch, flops, grid=()):
    moved = sum(a.size * a.dtype.itemsize for a in args) + sum(
        o.size * o.dtype.itemsize for o in outs
    )
    return pl.pallas_call(
        body,
        name=name,
        grid=grid,
        in_specs=specs,
        out_specs=[in_vmem(*o.shape) for o in outs],
        out_shape=outs,
        scratch_shapes=scratch,
        compiler_params=pltpu.CompilerParams(vmem_limit_bytes=GRANT),
        cost_estimate=pl.CostEstimate(flops=flops, bytes_accessed=moved, transcendentals=0),
    )(*args)


def activated(values, gain):
    mean = jnp.mean(values * values, axis=0, keepdims=True)
    scaled = values * lax.rsqrt(mean + 1e-06) * gain
    return scaled / (1.0 + jnp.exp(-scaled))


def rolled(value, step):
    count = value.shape[1]
    return value if step == 0 else pltpu.roll(value, step % count, 1)


def spread(columns, base, value, width, edged):
    depth, count = value.shape
    lane = lax.broadcasted_iota(jnp.int32, value.shape, 1)
    for j in range(3):
        moved = rolled(value, 1 - j)
        if edged and j == 0:
            moved = jnp.where(lane == 0, 0.0, moved)
        if edged and j == 2:
            moved = jnp.where(lane == count - 1, 0.0, moved)
        columns[base + j * depth : base + (j + 1) * depth, :] = moved[:, :width].astype(BF16)


def joined(c, own, other, whole):
    half = own.shape[0]
    whole[pl.ds(pl.multiple_of(c * half, half), half), :] = own.astype(F32)
    whole[pl.ds(pl.multiple_of((1 - c) * half, half), half), :] = other.astype(F32)
    return whole[...]


def low_cached_body(place, own, other, weights, total, columns, whole):
    frames, rows, half, _ = own.shape
    outs, depth = weights.shape[3:]
    total[...] = jnp.zeros_like(total)

    def row(r, _):
        for t in range(frames):
            value = joined(place[0], own[t, r], other[t, r], whole)
            spread(columns, t * 3 * depth, value, value.shape[1], True)
        sums = None
        for t in range(frames):
            left = jnp.concatenate(
                [weights[t, :, j].reshape(3 * outs, depth) for j in range(3)], axis=1
            )
            part = jnp.dot(
                left, columns[t * 3 * depth : (t + 1) * 3 * depth, :], preferred_element_type=F32
            )
            sums = part if sums is None else sums + part
        for i in range(3):
            total[r + 2 - i] += sums[i * outs : (i + 1) * outs]
        return 0

    lax.fori_loop(0, rows, row, 0)


def low_living_body(place, own, other, gain, cached, weights, inner, edges, total, columns, whole):
    rows, half, _ = own.shape
    outs, depth = weights.shape[3:]
    total[...] = cached[...]

    def row(r, _):
        value = joined(place[0], own[r], other[r], whole)
        value = activated(value, gain[...])
        spread(columns, 0, value, value.shape[1], True)
        left = jnp.concatenate(
            [weights[0, :, j].reshape(3 * outs, depth) for j in range(3)], axis=1
        )
        sums = jnp.dot(left, columns[...], preferred_element_type=F32)
        for i in range(3):
            total[r + 2 - i] += sums[i * outs : (i + 1) * outs]
        return 0

    lax.fori_loop(0, rows, row, 0)
    inner[...] = total[1 : rows + 1]
    edges[0] = total[0].astype(BF16)
    edges[1] = total[rows + 1].astype(BF16)


def low_cached(place, own, other, kernel):
    frames, rows, half, width = own.shape
    outs, depth = kernel.shape[3:]
    return call(
        low_cached_body,
        "low_cached",
        (place, own, other, kernel),
        [
            SCALAR,
            in_vmem(*own.shape),
            in_vmem(*other.shape),
            in_vmem(frames, 3, 3, outs, depth),
        ],
        [jax.ShapeDtypeStruct((rows + 2, outs, width), F32)],
        [pltpu.VMEM((frames * 3 * depth, width), BF16), pltpu.VMEM((depth, width), F32)],
        2 * frames * 9 * outs * depth * rows * width,
        (1,),
    )[0]


def low_living(place, own, other, gain, cached, kernel):
    rows, half, width = own.shape
    frames = kernel.shape[0]
    outs, depth = kernel.shape[3:]
    return call(
        low_living_body,
        "low_living",
        (place, own, other, gain, cached, kernel),
        [
            SCALAR,
            in_vmem(*own.shape),
            in_vmem(*other.shape),
            in_vmem(*gain.shape),
            in_vmem(*cached.shape),
            pl.BlockSpec((1, 3, 3, outs, depth), lambda _: (frames - 1, 0, 0, 0, 0)),
        ],
        [
            jax.ShapeDtypeStruct((rows, outs, width), F32),
            jax.ShapeDtypeStruct((2, outs, width), BF16),
        ],
        [
            pltpu.VMEM((rows + 2, outs, width), F32),
            pltpu.VMEM((3 * depth, width), BF16),
            pltpu.VMEM((depth, width), F32),
        ],
        2 * 9 * outs * depth * rows * width,
        (1,),
    )


def high_sums(total, first, sums, outs, share):
    for i in range(3):
        for s in range(outs // share):
            total[first + 2 - i, s * share : (s + 1) * share, :] += sums[
                (3 * s + i) * share : (3 * s + i + 1) * share
            ]


def left_of(weights, pieces, first, last):
    rows, lanes = weights.shape[0] // pieces, weights.shape[1]
    parts = []
    while first < last:
        piece, start = divmod(first, lanes)
        stop = min(lanes, start + last - first)
        parts.append(weights[piece * rows : (piece + 1) * rows, start:stop])
        first += stop - start
    return parts[0] if len(parts) == 1 else jnp.concatenate(parts, axis=1)


def kept_lanes(c, width, shape):
    lane = lax.broadcasted_iota(jnp.int32, shape, 1)
    count = shape[1]
    middle = (width + count) // 2
    return (lane < jnp.where(c == 0, middle, width)) | (lane >= jnp.where(c == 0, count, middle))


def high_cached_body(
    share, place, own_a, strip_a, own_b, strip_b, weights, sums_a, sums_b, up, down,
    total_a, total_b, columns_a, columns_b, whole,
):
    frames, rows, depth, width = own_a.shape
    count = width + strip_a.shape[3]
    c = place[0]
    keep = kept_lanes(c, width, (depth, count))
    total_a[...] = jnp.zeros_like(total_a)
    total_b[...] = jnp.zeros_like(total_b)
    pieces = weights.shape[0] // (3 * depth)
    long = frames * 3 * depth
    second = long + 6 * depth

    def row(r, _):
        for own, strip, columns, upto in (
            (own_a, strip_a, columns_a, count),
            (own_b, strip_b, columns_b, width),
        ):
            for t in range(frames):
                whole[:, :width] = own[t, r].astype(F32)
                whole[:, width:] = strip[t, r].astype(F32)
                value = jnp.where(keep, whole[...], 0.0)
                spread(columns, t * 3 * depth, value, upto, False)
        part = jnp.dot(left_of(weights, pieces, 0, long), columns_a[...], preferred_element_type=F32)
        high_sums(total_a, r, part, depth, share)
        part = jnp.dot(
            left_of(weights, pieces, second, second + long),
            columns_b[...],
            preferred_element_type=F32,
        )
        high_sums(total_b, r, part, depth, share)
        return 0

    lax.fori_loop(0, rows, row, 0)
    sums_a[...] = total_a[...]
    sums_b[...] = total_b[1 : rows + 1]
    block = 128
    for packet, first, edge in ((up, 0, 0), (down, rows, rows + 1)):
        place_at = 0
        for source, at in ((total_a, first), (total_a, first + 1), (total_b, edge)):
            for lane in range(0, source.shape[2], block):
                packet[place_at] = source[at, :, lane : lane + block].astype(BF16)
                place_at += 1


def high_cached(place, own_a, strip_a, own_b, strip_b, weights, share):
    frames, rows, depth, width = own_a.shape
    count = width + strip_a.shape[3]
    blocks = (2 * count + width) // 128
    args = (place, own_a, strip_a, own_b, strip_b, weights)
    return call(
        functools.partial(high_cached_body, share),
        "high_cached",
        args,
        [SCALAR] + [in_vmem(*a.shape) for a in args[1:]],
        [
            jax.ShapeDtypeStruct((rows + 2, depth, count), F32),
            jax.ShapeDtypeStruct((rows, depth, width), F32),
            jax.ShapeDtypeStruct((blocks, depth, 128), BF16),
            jax.ShapeDtypeStruct((blocks, depth, 128), BF16),
        ],
        [
            pltpu.VMEM((rows + 2, depth, count), F32),
            pltpu.VMEM((rows + 2, depth, width), F32),
            pltpu.VMEM((frames * 3 * depth, count), BF16),
            pltpu.VMEM((frames * 3 * depth, width), BF16),
            pltpu.VMEM((depth, count), F32),
        ],
        2 * frames * 9 * depth * depth * rows * (width + count),
    )


def high_living_body(
    share, place, own, other, above, below, gain_a, gain_b, sums_a, sums_b, from_above, from_below,
    weights, decoded, wide, total, total_a, total_b, resampled, columns_r, columns, whole,
):
    rows, half, low_width = own.shape
    high_rows, outs, width = decoded.shape
    count = sums_a.shape[2]
    c, first, last = place[0], place[1], place[2]
    depth = 2 * half
    pieces = weights.shape[0] // (3 * outs)
    long = 6 * outs
    keep = kept_lanes(c, width, (outs, count))

    lane = lax.broadcasted_iota(jnp.int32, (low_width, count), 1)
    source = lax.broadcasted_iota(jnp.int32, (low_width, count), 0)
    column = jnp.where((c == 1) & (lane >= (width + count) // 2), lane - count, lane) + c * width
    wide[...] = jnp.where(kept_lanes(c, width, column.shape) & (column // 2 == source), 1.0, 0.0).astype(BF16)

    total[...] = jnp.zeros_like(total)

    def low_row(value, m):
        value = jnp.dot(value, wide[...], preferred_element_type=F32)
        spread(columns_r, 0, value, count, False)
        part = jnp.dot(
            left_of(weights, pieces, 3 * long, 3 * long + 3 * depth),
            columns_r[...],
            preferred_element_type=F32,
        )
        for s in range(outs // share):
            at = pl.ds(s * share, share)
            p0, p1, p2 = (
                part[(3 * s + i) * share : (3 * s + i + 1) * share] for i in range(3)
            )
            total[2 * m, at, :] += p2
            total[2 * m + 1, at, :] += p1 + p2
            total[2 * m + 2, at, :] += p0 + p1
            total[2 * m + 3, at, :] += p0

    def near(m, _):
        low_row(joined(c, own[m], other[m], whole).astype(BF16), m + rows)
        return 0

    def far(m, _):
        low_row(above[m], m)
        low_row(below[m], m + 2 * rows)
        return 0

    lax.fori_loop(0, rows, near, 0)
    lax.fori_loop(0, rows, far, 0)

    spare = 2 * rows - 1
    total_a[...] = jnp.zeros_like(total_a)
    total_a[2 : high_rows + 4] = sums_a[...]
    total_b[...] = jnp.zeros_like(total_b)
    total_b[2 : high_rows + 2] = sums_b[...]
    block = 128
    for packet, at_a, at_b in ((from_above, 2, 2), (from_below, high_rows + 2, high_rows + 1)):
        spot = 0
        for target, at in ((total_a, at_a), (total_a, at_a + 1), (total_b, at_b)):
            for start in range(0, target.shape[2], block):
                target[at, :, start : start + block] += packet[spot].astype(F32)
                spot += 1

    columns[...] = jnp.zeros_like(columns)
    pad = columns.shape[0] - 3 * outs

    def high_a(h, _):
        outside = ((first == 1) & (h < 2)) | ((last == 1) & (h >= high_rows + 2))
        value = jnp.where(keep, total[h + spare], 0.0).astype(BF16)
        value = jnp.where(outside, jnp.zeros_like(value), value)
        resampled[h] = value
        value = activated(value.astype(F32), gain_a[...])
        spread(columns, 0, value, count, False)
        part = jnp.dot(
            left_of(weights, pieces, long, long + columns.shape[0]), columns[...], preferred_element_type=F32
        )
        high_sums(total_a, h, part, outs, share)
        return 0

    lax.fori_loop(0, high_rows + 4, high_a, 0)
    columns[:pad, :] = jnp.zeros((pad, count), BF16)

    def high_b(h, _):
        outside = ((first == 1) & (h < 1)) | ((last == 1) & (h >= high_rows + 1))
        value = jnp.where(keep, total_a[h + 2], 0.0).astype(BF16)
        value = jnp.where(outside, jnp.zeros_like(value), value)
        value = activated(value.astype(F32), gain_b[...])
        for j in range(3):
            moved = rolled(value, 1 - j)
            columns[pad + j * outs : pad + (j + 1) * outs, :width] = moved[:, :width].astype(BF16)
        part = jnp.dot(
            left_of(weights, pieces, 2 * long - columns.shape[0], 2 * long),
            columns[:, :width],
            preferred_element_type=F32,
        )
        high_sums(total_b, h, part, outs, share)
        return 0

    lax.fori_loop(0, high_rows + 2, high_b, 0)
    for h in range(high_rows):
        decoded[h] = (total_b[h + 2] + resampled[h + 2, :, :width].astype(F32)).astype(BF16)


def high_living(
    place, own, other, above, below, gain_a, gain_b, sums_a, sums_b, from_above, from_below,
    weights, share,
):
    rows, half, low_width = own.shape
    high_rows, outs, width = sums_b.shape
    count = sums_a.shape[2]
    depth = 2 * half
    args = (
        place, own, other, above, below, gain_a, gain_b, sums_a, sums_b, from_above, from_below,
        weights,
    )
    padded = -(-3 * outs // 128) * 128
    return call(
        functools.partial(high_living_body, share),
        "high_living",
        args,
        [SCALAR] + [in_vmem(*a.shape) for a in args[1:]],
        [jax.ShapeDtypeStruct((high_rows, outs, width), BF16)],
        [
            pltpu.VMEM((low_width, count), BF16),
            pltpu.VMEM((6 * rows + 2, outs, count), F32),
            pltpu.VMEM((high_rows + 6, outs, count), F32),
            pltpu.VMEM((high_rows + 4, outs, width), F32),
            pltpu.VMEM((high_rows + 4, outs, count), BF16),
            pltpu.VMEM((3 * depth, count), BF16),
            pltpu.VMEM((padded, count), BF16),
            pltpu.VMEM((depth, low_width), F32),
        ],
        2 * 27 * outs * outs * high_rows * width + 2 * 9 * outs * depth * high_rows * count,
    )[0]


def body(
    latent,
    cache_low_a,
    cache_low_b,
    gain_low_a,
    gain_low_b,
    kernel_low_a,
    kernel_low_b,
    resample_kernel,
    gain_high_a,
    gain_high_b,
    kernel_high_a,
    kernel_high_b,
    cache_high_a,
    cache_high_b,
):
    c = lax.axis_index("chan")
    r = lax.axis_index("rows")
    row_count = lax.axis_size("rows")
    swap = [(0, 1), (1, 0)]

    def other_half(value):
        return lax.ppermute(value, "chan", swap)

    def downward(value):
        return lax.ppermute(value, "rows", [(i, i + 1) for i in range(row_count - 1)])

    def upward(value):
        return lax.ppermute(value, "rows", [(i + 1, i) for i in range(row_count - 1)])

    place = jnp.stack([c, r == 0, r == row_count - 1]).astype(jnp.int32)

    share = kernel_high_a.shape[3]

    def flat(kernel):
        turned = jnp.transpose(kernel, (1, 3, 0, 2, 4))
        return turned.reshape(3 * share, -1)

    flat_a, flat_b = flat(kernel_high_a), flat(kernel_high_b)
    flat_r = flat(resample_kernel[None])
    outs = kernel_high_a.shape[4]
    long = 6 * outs
    lined = jnp.concatenate([flat_a, flat_b[:, long:], flat_b[:, :long], flat_r], axis=1)
    pieces = lax.axis_size("views")
    lanes = -(-lined.shape[1] // (128 * pieces)) * 128
    lined = jnp.pad(lined, ((0, 0), (0, lanes * pieces - lined.shape[1])))
    mine = lax.dynamic_slice_in_dim(lined, lax.axis_index("views") * lanes, lanes, 1)
    weights = lax.all_gather(mine, ("views", "rows"), axis=0, tiled=True)
    if share % 8:
        weights = weights.reshape(pieces, -1, 3, share, lanes).transpose(0, 2, 1, 3, 4)
        weights = weights.reshape(-1, lanes)
        share = outs

    def column_of(gain, other):
        return jnp.where(
            c == 0, jnp.concatenate([gain, other]), jnp.concatenate([other, gain])
        ).astype(F32)[:, None]

    other_latent = other_half(latent)
    gains = jnp.stack([gain_low_a, gain_low_b])
    other_gains = other_half(gains)
    other_cache_a = other_half(cache_low_a)
    other_cache_b = other_half(cache_low_b)
    width = cache_high_a.shape[3]
    strip = 128
    edge = [
        lax.dynamic_slice_in_dim(cache, (1 - c) * (width - strip), strip, 3)
        for cache in (cache_high_a, cache_high_b)
    ]
    strips = other_half(jnp.stack(edge))

    def level1_conv(inputs, other, cached, gain, kernel):
        inner, edges = low_living(place, inputs, other, gain, cached, kernel)
        from_above = downward(edges[1])
        from_below = upward(edges[0])
        rest = jnp.zeros((inner.shape[0] - 2, *from_above.shape), BF16)
        added = jnp.concatenate([from_above[None], rest, from_below[None]])
        return inner + added.astype(F32)

    cached_a = low_cached(place, cache_low_a, other_cache_a, kernel_low_a)
    cached_b = low_cached(place, cache_low_b, other_cache_b, kernel_low_b)
    middle_low = level1_conv(
        latent, other_latent, cached_a, column_of(gains[0], other_gains[0]), kernel_low_a
    ).astype(BF16)
    level_one = (
        latent.astype(F32)
        + level1_conv(
            middle_low,
            other_half(middle_low),
            cached_b,
            column_of(gains[1], other_gains[1]),
            kernel_low_b,
        )
    ).astype(BF16)
    other_one = other_half(level_one)
    both = jnp.where(
        c == 0,
        jnp.concatenate([level_one, other_one], axis=1),
        jnp.concatenate([other_one, level_one], axis=1),
    )
    above, below = downward(both), upward(both)

    sums_a, sums_b, up, down = high_cached(
        place, cache_high_a, strips[0], cache_high_b, strips[1], weights, share
    )
    from_above, from_below = downward(down), upward(up)
    return high_living(
        place,
        level_one,
        other_one,
        above,
        below,
        gain_high_a.astype(F32)[:, None],
        gain_high_b.astype(F32)[:, None],
        sums_a,
        sums_b,
        from_above,
        from_below,
        weights,
        share,
    )


def solution(mesh):
    placed = (
        P(("views", "rows"), "chan", None),
        P(None, ("views", "rows"), "chan", None),
        P(None, ("views", "rows"), "chan", None),
        P("chan"),
        P("chan"),
        P(None, None, None, "chan", None),
        P(None, None, None, "chan", None),
        P(None, None, "rows", None),
        P(),
        P(),
        P(None, None, None, "rows", None),
        P(None, None, None, "rows", None),
        P(None, ("views", "rows"), None, "chan"),
        P(None, ("views", "rows"), None, "chan"),
    )
    return jax.shard_map(
        body,
        mesh=mesh,
        in_specs=placed,
        out_specs=P(("views", "rows"), None, "chan"),
        check_vma=False,
    )
```

```python
import functools

import jax
import jax.numpy as jnp
from jax import lax
from jax.experimental import pallas as pl
from jax.experimental.pallas import tpu as pltpu
from jax.sharding import PartitionSpec as P

F32, BF16 = jnp.float32, jnp.bfloat16
MIB = 1024 * 1024


def in_vmem(*shape):
    return pl.BlockSpec(memory_space=pltpu.VMEM)


SCALAR = pl.BlockSpec(memory_space=pltpu.SMEM)


def size_of(shaped):
    rows = -(-shaped.shape[-2] // 16) * 16
    lanes = -(-shaped.shape[-1] // 128) * 128
    lead = 1
    for extent in shaped.shape[:-2]:
        lead *= extent
    return lead * rows * lanes * jnp.dtype(shaped.dtype).itemsize


def call(body, name, args, outs, scratch, flops):
    moved = sum(size_of(a) for a in args[1:]) + sum(size_of(o) for o in outs)
    held = moved + sum(size_of(jax.ShapeDtypeStruct(s.shape, s.dtype)) for s in scratch)
    return pl.pallas_call(
        body,
        name=name,
        in_specs=[SCALAR] + [in_vmem()] * (len(args) - 1),
        out_specs=[in_vmem()] * len(outs),
        out_shape=outs,
        scratch_shapes=scratch,
        compiler_params=pltpu.CompilerParams(vmem_limit_bytes=held + 4 * MIB),
        cost_estimate=pl.CostEstimate(flops=flops, bytes_accessed=moved, transcendentals=0),
    )(*args)


def silu_of(values, scale, gain):
    scaled = values * scale * gain
    return scaled / (1.0 + jnp.exp(-scaled))


def activated(values, gain):
    mean = jnp.mean(values * values, axis=0, keepdims=True)
    return silu_of(values, lax.rsqrt(mean + 1e-06), gain)


def column_of(gains, row):
    count = gains.shape[1]
    same = lax.broadcasted_iota(jnp.int32, (count, count), 0) == lax.broadcasted_iota(
        jnp.int32, (count, count), 1
    )
    turned = lax.dot_general(
        jnp.where(same, 1.0, 0.0).astype(BF16),
        gains,
        (((1,), (1,)), ((), ())),
        preferred_element_type=F32,
    )
    return turned[:, row : row + 1]


def rolled(value, step):
    count = value.shape[1]
    return value if step == 0 else pltpu.roll(value, step % count, 1)


def in_order(c, own, other):
    return jnp.where(c == 0, own, other), jnp.where(c == 0, other, own)


def spread(columns, base, stride, value, width, edged):
    depth, count = value.shape
    lane = lax.broadcasted_iota(jnp.int32, value.shape, 1)
    for j in range(3):
        moved = rolled(value, 1 - j)
        if edged and j == 0:
            moved = jnp.where(lane == 0, 0.0, moved)
        if edged and j == 2:
            moved = jnp.where(lane == count - 1, 0.0, moved)
        at = base + j * stride
        columns[at : at + depth, :] = moved[:, :width].astype(BF16)


def in_turn(count, fill, use, buffers):
    fill(0, buffers[0])

    def pair(k, _):
        for side in range(2):
            step = 2 * k + side
            fill(jnp.minimum(step + 1, count - 1), buffers[1 - side])
            use(step, buffers[side])
        return 0

    lax.fori_loop(0, count // 2, pair, 0)
    if count % 2:
        use(count - 1, buffers[0])


def low_sums(total, r, weights, first, frames, columns):
    outs, depth = weights.shape[3:]
    for i in range(3):
        sums = None
        for t in range(frames):
            left = jnp.concatenate([weights[first + t, i, j] for j in range(3)], axis=1)
            part = jnp.dot(
                left, columns[t * 3 * depth : (t + 1) * 3 * depth, :], preferred_element_type=F32
            )
            sums = part if sums is None else sums + part
        total[r + 2 - i] += sums


def low_cached_body(place, own, other, weights, total, *buffers):
    frames, rows, half, width = own.shape
    depth = 2 * half
    c = place[0]
    total[...] = jnp.zeros_like(total)

    def fill(r, columns):
        for t in range(frames):
            for at, value in enumerate(in_order(c, own[t, r], other[t, r])):
                base = t * 3 * depth + at * half
                spread(columns, base, depth, value.astype(F32), width, True)

    def use(r, columns):
        low_sums(total, r, weights, 0, frames, columns)

    in_turn(rows, fill, use, buffers)


def low_living_body(
    which, place, own, other, gain, other_gain, cached, weights, inner, red, black, total, *buffers
):
    rows, half, width = own.shape
    depth = 2 * half
    c, even = place[0], place[3]
    total[...] = cached[...]
    mine = column_of(gain[...], which)
    theirs = column_of(other_gain[...], which)

    def fill(r, columns):
        a, b = own[r].astype(F32), other[r].astype(F32)
        squares = jnp.sum(a * a, axis=0, keepdims=True) + jnp.sum(b * b, axis=0, keepdims=True)
        scale = lax.rsqrt(squares / depth + 1e-06)
        a, b = in_order(c, silu_of(a, scale, mine), silu_of(b, scale, theirs))
        spread(columns, 0, depth, a, width, True)
        spread(columns, half, depth, b, width, True)

    def use(r, columns):
        low_sums(total, r, weights, weights.shape[0] - 1, 1, columns)

    in_turn(rows, fill, use, buffers)
    inner[...] = total[1 : rows + 1]
    up, down = total[0].astype(BF16), total[rows + 1].astype(BF16)
    red[...] = jnp.where(even == 1, down, up)
    black[...] = jnp.where(even == 1, up, down)


def low_cached(place, own, other, kernel):
    frames, rows, half, width = own.shape
    outs, depth = kernel.shape[3:]
    return call(
        low_cached_body,
        "low_cached",
        (place, own, other, kernel),
        [jax.ShapeDtypeStruct((rows + 2, outs, width), F32)],
        [pltpu.VMEM((frames * 3 * depth, width), BF16)] * 2,
        2 * frames * 9 * outs * depth * rows * width,
    )[0]


def low_living(place, own, other, gain, other_gain, which, cached, kernel):
    rows, half, width = own.shape
    outs, depth = kernel.shape[3:]
    return call(
        functools.partial(low_living_body, which),
        "low_living",
        (place, own, other, gain, other_gain, cached, kernel),
        [
            jax.ShapeDtypeStruct((rows, outs, width), F32),
            jax.ShapeDtypeStruct((outs, width), BF16),
            jax.ShapeDtypeStruct((outs, width), BF16),
        ],
        [pltpu.VMEM((rows + 2, outs, width), F32)]
        + [pltpu.VMEM((3 * depth, width), BF16)] * 2,
        2 * 9 * outs * depth * rows * width,
    )


def one_hot(condition):
    return jnp.where(condition, 1.0, 0.0).astype(BF16)


def edge_body(place, cache_a, cache_b, packet):
    frames, rows, depth, width = cache_a.shape
    c = place[0]
    source = lax.broadcasted_iota(jnp.int32, (width, 128), 0)
    lane = lax.broadcasted_iota(jnp.int32, (width, 128), 1)
    start = jnp.where(c == 0, width - 2, 0)
    near = jnp.where(c == 0, width - 1, 0)
    sums = jnp.zeros((depth, 128), F32)
    for t in range(frames):
        for r in range(rows):
            k = lane - 2 * (t * rows + r)
            pick = one_hot((k >= 0) & (k < 2) & (source == start + k))
            sums += jnp.dot(cache_a[t, r], pick, preferred_element_type=F32)
            at = 2 * frames * rows + t * rows + r
            pick = one_hot((lane == at) & (source == near))
            sums += jnp.dot(cache_b[t, r], pick, preferred_element_type=F32)
    packet[...] = sums.astype(BF16)


def edges_of(place, cache_a, cache_b):
    frames, rows, depth, _ = cache_a.shape
    return call(
        edge_body,
        "edges",
        (place, cache_a, cache_b),
        [jax.ShapeDtypeStruct((depth, 128), BF16)],
        [],
        4 * frames * rows * depth * 256 * 128,
    )[0]


def close_body(place, latent, inner, red, black, kept, kept_edge, sent):
    rows, outs, width = latent.shape
    span = width // 2
    c, even = place[0], place[3]
    source = lax.broadcasted_iota(jnp.int32, (width, 128), 0)
    lane = lax.broadcasted_iota(jnp.int32, (width, 128), 1)
    mine = jnp.where(c == 0, span, span - 2)
    theirs = jnp.where(c == 0, span - 2, span)
    edge_mine = jnp.zeros((outs, 128), F32)
    edge_theirs = jnp.zeros((outs, 128), F32)
    for r in range(rows):
        value = latent[r].astype(F32) + inner[r]
        if r == 0:
            value += jnp.where(even == 1, black[...], red[...]).astype(F32)
        if r == rows - 1:
            value += jnp.where(even == 1, red[...], black[...]).astype(F32)
        value = value.astype(BF16)
        left, right = value[:, :span], value[:, span:]
        kept[r] = jnp.where(c == 0, left, right)
        sent[r] = jnp.where(c == 0, right, left)
        k = lane - 2 * (c * rows + r)
        inside = (k >= 0) & (k < 2)
        edge_mine += jnp.dot(
            value, one_hot(inside & (source == mine + k)), preferred_element_type=F32
        )
        edge_theirs += jnp.dot(
            value, one_hot(inside & (source == theirs + k)), preferred_element_type=F32
        )
    kept_edge[...] = edge_mine.astype(BF16)
    sent[rows] = edge_theirs.astype(BF16)


def close(place, latent, inner, red, black):
    rows, outs, width = latent.shape
    span = width // 2
    return call(
        close_body,
        "close",
        (place, latent, inner, red, black),
        [
            jax.ShapeDtypeStruct((rows, outs, span), BF16),
            jax.ShapeDtypeStruct((outs, 128), BF16),
            jax.ShapeDtypeStruct((rows + 1, outs, span), BF16),
        ],
        [],
        4 * rows * outs * width * 128,
    )


def high_sums(total, first, weights, lanes, columns, width, share):
    outs = total.shape[1]
    group = min(2, outs // share)
    for s in range(0, outs // share, group):
        rows = slice(3 * s * share, 3 * (s + group) * share)
        part = jnp.dot(
            left_of(weights, 3 * outs, rows, *lanes), columns[:, :width], preferred_element_type=F32
        )
        for g in range(group):
            for i in range(3):
                at = 3 * g + i
                total[first + 2 - i, (s + g) * share : (s + g + 1) * share, :] += part[
                    at * share : (at + 1) * share
                ]


def left_of(weights, height, rows, first, last):
    lanes = weights.shape[1]
    parts = []
    while first < last:
        piece, start = divmod(first, lanes)
        stop = min(lanes, start + last - first)
        parts.append(weights[piece * height + rows.start : piece * height + rows.stop, start:stop])
        first += stop - start
    return parts[0] if len(parts) == 1 else jnp.concatenate(parts, axis=1)


def kept_lanes(c, width, shape):
    lane = lax.broadcasted_iota(jnp.int32, shape, 1)
    count = shape[1]
    middle = (width + count) // 2
    return (lane < jnp.where(c == 0, middle, width)) | (lane >= jnp.where(c == 0, count, middle))


def high_cached_body(
    share, place, own_a, own_b, edge, weights, sums_a, sums_b, red, black, total_a, total_b,
    columns_a0, columns_a1, columns_b0, columns_b1,
):
    frames, rows, depth, width = own_a.shape
    count = total_a.shape[2]
    c, even = place[0], place[3]
    total_a[...] = jnp.zeros_like(total_a)
    total_b[...] = jnp.zeros_like(total_b)
    long = frames * 3 * depth
    second = long + 6 * depth
    lane = lax.broadcasted_iota(jnp.int32, (depth, 128), 1)

    def fill(r, columns):
        for t in range(frames):
            at = t * rows + r
            first = jnp.where(c == 0, 0, 126)
            moved = pltpu.roll(edge[...].astype(F32), (first - 2 * at + 256) % 128, 1)
            beside = jnp.where((lane >= first) & (lane < first + 2), moved, 0.0)
            value = jnp.concatenate([own_a[t, r].astype(F32), beside], axis=1)
            spread(columns[0], t * 3 * depth, depth, value, count, False)
            at += 2 * frames * rows
            first = jnp.where(c == 0, 0, 127)
            moved = pltpu.roll(edge[...].astype(F32), (first - at + 256) % 128, 1)
            beside = jnp.where(lane == first, moved, 0.0)
            value = jnp.concatenate([own_b[t, r].astype(F32), beside], axis=1)
            spread(columns[1], t * 3 * depth, depth, value, width, False)

    def use(r, columns):
        high_sums(total_a, r, weights, (0, long), columns[0], count, share)
        high_sums(total_b, r, weights, (second, second + long), columns[1], width, share)

    in_turn(rows, fill, use, ((columns_a0, columns_b0), (columns_a1, columns_b1)))
    sums_a[...] = total_a[...]
    sums_b[...] = total_b[1 : rows + 1]
    spot = 0
    for source, top, bottom in (
        (total_a, 0, rows), (total_a, 1, rows + 1), (total_b, 0, rows + 1)
    ):
        for start in range(0, source.shape[2], 128):
            lanes = slice(start, start + 128)
            up, down = source[top, :, lanes].astype(BF16), source[bottom, :, lanes].astype(BF16)
            red[spot] = jnp.where(even == 1, down, up)
            black[spot] = jnp.where(even == 1, up, down)
            spot += 1


def high_cached(place, own_a, own_b, edge, weights, share):
    frames, rows, depth, width = own_a.shape
    count = width + 128
    blocks = (2 * count + width) // 128
    return call(
        functools.partial(high_cached_body, share),
        "high_cached",
        (place, own_a, own_b, edge, weights),
        [
            jax.ShapeDtypeStruct((rows + 2, depth, count), F32),
            jax.ShapeDtypeStruct((rows, depth, width), F32),
            jax.ShapeDtypeStruct((blocks, depth, 128), BF16),
            jax.ShapeDtypeStruct((blocks, depth, 128), BF16),
        ],
        [
            pltpu.VMEM((rows + 2, depth, count), F32),
            pltpu.VMEM((rows + 2, depth, width), F32),
        ]
        + [pltpu.VMEM((frames * 3 * depth, count), BF16)] * 2
        + [pltpu.VMEM((frames * 3 * depth, width), BF16)] * 2,
        2 * frames * 9 * depth * depth * rows * (width + count),
    )


def high_living_body(
    share, place, one, above, below, gain_a, gain_b, sums_a, sums_b, red, black, weights, decoded,
    wide, total, total_a, total_b, resampled, columns_r0, columns_r1, columns_0, columns_1,
):
    blocks, half, span = one.shape
    rows = (blocks - 1) // 2
    high_rows, outs, width = decoded.shape
    count = sums_a.shape[2]
    c, first, last, even = place[0], place[1], place[2], place[3]
    depth = 2 * half
    long = 6 * outs
    keep = kept_lanes(c, width, (outs, count))

    lane = lax.broadcasted_iota(jnp.int32, (span + 128, count), 1)
    source = lax.broadcasted_iota(jnp.int32, (span + 128, count), 0)
    column = jnp.where((c == 1) & (lane >= (width + count) // 2), lane - count, lane) + c * width
    low = column >> 1
    inside = low - c * span
    k = low - jnp.where(c == 0, span, span - 2)
    own_lane = (source == inside) & (inside < span)
    for g in range(2):
        for r in range(rows):
            edge_lane = (source == span + 2 * (g * rows + r) + k) & (k >= 0) & (k < 2)
            edge_lane = edge_lane & ((inside < 0) | (inside >= span))
            spot = kept_lanes(c, width, column.shape) & (own_lane | edge_lane)
            wide[g * rows + r] = one_hot(spot)

    total[...] = jnp.zeros_like(total)

    def fill_low(tile, r, columns):
        for at, value in enumerate(in_order(c, tile[r], tile[rows + r])):
            value = jnp.concatenate([value, tile[2 * rows]], axis=1)
            value = jnp.dot(value, wide[at * rows + r], preferred_element_type=F32)
            spread(columns, at * half, depth, value, count, False)

    def use_low(m, columns):
        group = min(2, outs // share)
        for s in range(0, outs // share, group):
            picked = slice(3 * s * share, 3 * (s + group) * share)
            part = jnp.dot(
                left_of(weights, 3 * outs, picked, 3 * long, 3 * long + 3 * depth),
                columns[...],
                preferred_element_type=F32,
            )
            for g in range(group):
                at = slice((s + g) * share, (s + g + 1) * share)
                p0, p1, p2 = (
                    part[(3 * g + i) * share : (3 * g + i + 1) * share] for i in range(3)
                )
                total[2 * m, at, :] += p2
                total[2 * m + 1, at, :] += p1 + p2
                total[2 * m + 2, at, :] += p0 + p1
                total[2 * m + 3, at, :] += p0

    buffers = (columns_r0, columns_r1)
    steps = [(one, rows)] + [(above, 0)] + [(below, 2 * rows)]
    steps = [(tile, r, at + r) for tile, at in steps for r in range(rows)]
    fill_low(steps[0][0], steps[0][1], buffers[0])
    for k, (tile, r, at) in enumerate(steps):
        if k + 1 < len(steps):
            fill_low(steps[k + 1][0], steps[k + 1][1], buffers[(k + 1) % 2])
        use_low(at, buffers[k % 2])

    spare = 2 * rows - 1
    total_a[...] = jnp.zeros_like(total_a)
    total_a[2 : high_rows + 4] = sums_a[...]
    total_b[...] = jnp.zeros_like(total_b)
    total_b[2 : high_rows + 2] = sums_b[...]
    spot = 0
    for target, top, bottom in (
        (total_a, 2, high_rows + 2), (total_a, 3, high_rows + 3), (total_b, 2, high_rows + 1)
    ):
        for start in range(0, target.shape[2], 128):
            lanes = slice(start, start + 128)
            a, b = red[spot].astype(F32), black[spot].astype(F32)
            target[top, :, lanes] += jnp.where(even == 1, b, a)
            target[bottom, :, lanes] += jnp.where(even == 1, a, b)
            spot += 1

    buffers = (columns_0, columns_1)
    pad = columns_0.shape[0] - 3 * outs
    for columns in buffers:
        columns[3 * outs :, :] = jnp.zeros((pad, count), BF16)
    left_a, left_b = column_of(gain_a[...], 0), column_of(gain_b[...], 0)

    def fill_a(h, columns):
        outside = ((first == 1) & (h < 2)) | ((last == 1) & (h >= high_rows + 2))
        value = jnp.where(keep, total[h + spare], 0.0).astype(BF16)
        value = jnp.where(outside, jnp.zeros_like(value), value)
        resampled[h] = value
        spread(columns, 0, outs, activated(value.astype(F32), left_a), count, False)

    def use_a(h, columns):
        high_sums(
            total_a, h, weights, (long, long + columns.shape[0]), columns, count, share
        )

    in_turn(high_rows + 4, fill_a, use_a, buffers)
    for columns in buffers:
        columns[:pad, :] = jnp.zeros((pad, count), BF16)

    def fill_b(h, columns):
        outside = ((first == 1) & (h < 1)) | ((last == 1) & (h >= high_rows + 1))
        value = jnp.where(keep, total_a[h + 2], 0.0).astype(BF16)
        value = jnp.where(outside, jnp.zeros_like(value), value)
        spread(columns, pad, outs, activated(value.astype(F32), left_b), count, False)

    def use_b(h, columns):
        high_sums(
            total_b, h, weights, (2 * long - columns.shape[0], 2 * long), columns, width, share
        )

    in_turn(high_rows + 2, fill_b, use_b, buffers)
    for h in range(high_rows):
        decoded[h] = (total_b[h + 2] + resampled[h + 2, :, :width].astype(F32)).astype(BF16)


def high_living(
    place, one, above, below, gain_a, gain_b, sums_a, sums_b, red, black, weights, share
):
    blocks, half, span = one.shape
    rows = (blocks - 1) // 2
    high_rows, outs, width = sums_b.shape
    count = sums_a.shape[2]
    depth = 2 * half
    padded = -(-3 * outs // 128) * 128
    return call(
        functools.partial(high_living_body, share),
        "high_living",
        (place, one, above, below, gain_a, gain_b, sums_a, sums_b, red, black, weights),
        [jax.ShapeDtypeStruct((high_rows, outs, width), BF16)],
        [
            pltpu.VMEM((2 * rows, span + 128, count), BF16),
            pltpu.VMEM((6 * rows + 2, outs, count), F32),
            pltpu.VMEM((high_rows + 6, outs, count), F32),
            pltpu.VMEM((high_rows + 4, outs, width), F32),
            pltpu.VMEM((high_rows + 4, outs, count), BF16),
        ]
        + [pltpu.VMEM((3 * depth, count), BF16)] * 2
        + [pltpu.VMEM((padded, count), BF16)] * 2,
        2 * 27 * outs * outs * high_rows * width + 2 * 9 * outs * depth * high_rows * count,
    )[0]


def body(
    latent,
    cache_low_a,
    cache_low_b,
    gain_low_a,
    gain_low_b,
    kernel_low_a,
    kernel_low_b,
    resample_kernel,
    gain_high_a,
    gain_high_b,
    kernel_high_a,
    kernel_high_b,
    cache_high_a,
    cache_high_b,
):
    c = lax.axis_index("chan")
    r = lax.axis_index("rows")
    row_count = lax.axis_size("rows")
    swap = [(0, 1), (1, 0)]

    def other_half(value):
        return lax.ppermute(value, "chan", swap)

    reds = [(i, i ^ 1) for i in range(row_count) if i ^ 1 < row_count]
    blacks = [(i, i + 1 if i % 2 else i - 1) for i in range(1, row_count - 1 + row_count % 2)]

    def by_red(value):
        return lax.ppermute(value, "rows", reds)

    def by_black(value):
        return lax.ppermute(value, "rows", blacks)

    even = r % 2 == 0
    place = jnp.stack([c, r == 0, r == row_count - 1, even]).astype(jnp.int32)

    share = kernel_high_a.shape[3]

    def flat(kernel):
        turned = jnp.transpose(kernel, (1, 3, 0, 2, 4))
        return turned.reshape(3 * share, -1)

    flat_a, flat_b = flat(kernel_high_a), flat(kernel_high_b)
    flat_r = flat(resample_kernel[None])
    outs = kernel_high_a.shape[4]
    long = 6 * outs
    lined = jnp.concatenate([flat_a, flat_b[:, long:], flat_b[:, :long], flat_r], axis=1)
    pieces = lax.axis_size("views")
    lanes = -(-lined.shape[1] // (128 * pieces)) * 128
    lined = jnp.pad(lined, ((0, 0), (0, lanes * pieces - lined.shape[1])))
    mine = lax.dynamic_slice_in_dim(lined, lax.axis_index("views") * lanes, lanes, 1)
    weights = lax.all_gather(mine, ("views", "rows"), axis=0, tiled=True)
    if share % 8:
        weights = weights.reshape(pieces, -1, 3, share, lanes).transpose(0, 2, 1, 3, 4)
        weights = weights.reshape(-1, lanes)
        share = outs

    rows, half, low_width = latent.shape
    gains = jnp.pad(jnp.stack([gain_low_a, gain_low_b]), ((0, 14), (0, 0)))
    sent = jnp.pad(gains, ((0, 0), (0, low_width - half)))
    sent = jnp.concatenate([latent.reshape(rows * half, low_width), sent])
    got = other_half(sent)
    other_latent = got[: rows * half].reshape(latent.shape)
    other_gains = got[rows * half :, :half]
    other_cache_a = other_half(cache_low_a)
    other_cache_b = other_half(cache_low_b)
    edge = other_half(edges_of(place, cache_high_a, cache_high_b))

    def low_conv(inputs, other, cached, which, kernel):
        inner, red, black = low_living(
            place, inputs, other, gains, other_gains, which, cached, kernel
        )
        return inner, by_red(red), by_black(black)

    cached_a = low_cached(place, cache_low_a, other_cache_a, kernel_low_a)
    cached_b = low_cached(place, cache_low_b, other_cache_b, kernel_low_b)
    inner, red, black = low_conv(latent, other_latent, cached_a, 0, kernel_low_a)
    top = jnp.where(even, black, red).astype(F32)
    bottom = jnp.where(even, red, black).astype(F32)
    middle_low = jnp.concatenate(
        [inner[:1] + top, inner[1:-1], inner[-1:] + bottom]
    ).astype(BF16)
    inner, red, black = low_conv(middle_low, other_half(middle_low), cached_b, 1, kernel_low_b)
    kept, kept_edge, sent = close(place, latent, inner, red, black)
    got = other_half(sent)
    one = jnp.concatenate([kept, got[:rows], (kept_edge + got[rows])[None]])
    from_red, from_black = by_red(one), by_black(one)
    above = jnp.where(even, from_black, from_red)
    below = jnp.where(even, from_red, from_black)

    sums_a, sums_b, red, black = high_cached(
        place, cache_high_a, cache_high_b, edge, weights, share
    )
    return high_living(
        place,
        one,
        above,
        below,
        jnp.pad(gain_high_a[None], ((0, 15), (0, 0))),
        jnp.pad(gain_high_b[None], ((0, 15), (0, 0))),
        sums_a,
        sums_b,
        by_red(red),
        by_black(black),
        weights,
        share,
    )


def solution(mesh):
    placed = (
        P(("views", "rows"), "chan", None),
        P(None, ("views", "rows"), "chan", None),
        P(None, ("views", "rows"), "chan", None),
        P("chan"),
        P("chan"),
        P(None, None, None, "chan", None),
        P(None, None, None, "chan", None),
        P(None, None, "rows", None),
        P(),
        P(),
        P(None, None, None, "rows", None),
        P(None, None, None, "rows", None),
        P(None, ("views", "rows"), None, "chan"),
        P(None, ("views", "rows"), None, "chan"),
    )
    return jax.shard_map(
        body,
        mesh=mesh,
        in_specs=placed,
        out_specs=P(("views", "rows"), None, "chan"),
        check_vma=False,
    )
```

```python
import functools

import jax
import jax.numpy as jnp
from jax import lax
from jax.experimental import pallas as pl
from jax.experimental.pallas import tpu as pltpu
from jax.sharding import PartitionSpec as P

F32, BF16 = jnp.float32, jnp.bfloat16
MIB = 1024 * 1024


def in_vmem(*shape):
    return pl.BlockSpec(memory_space=pltpu.VMEM)


SCALAR = pl.BlockSpec(memory_space=pltpu.SMEM)


def size_of(shaped):
    rows = -(-shaped.shape[-2] // 16) * 16
    lanes = -(-shaped.shape[-1] // 128) * 128
    lead = 1
    for extent in shaped.shape[:-2]:
        lead *= extent
    return lead * rows * lanes * jnp.dtype(shaped.dtype).itemsize


def call(body, name, args, outs, scratch, flops, far=(), grant=None):
    moved = sum(size_of(a) for a in args[1:]) + sum(size_of(o) for o in outs)
    held = moved + sum(
        size_of(jax.ShapeDtypeStruct(s.shape, s.dtype)) for s in scratch if len(s.shape) > 1
    )
    return pl.pallas_call(
        body,
        name=name,
        in_specs=[SCALAR]
        + [in_vmem()] * (len(args) - 1)
        + [pl.BlockSpec(memory_space=pltpu.HBM)] * len(far),
        out_specs=[in_vmem()] * len(outs),
        out_shape=outs,
        scratch_shapes=scratch,
        compiler_params=pltpu.CompilerParams(vmem_limit_bytes=grant or held + 4 * MIB),
        cost_estimate=pl.CostEstimate(flops=flops, bytes_accessed=moved, transcendentals=0),
    )(*args, *far)


def silu_of(values, scale, gain):
    scaled = values * scale * gain
    return scaled / (1.0 + jnp.exp(-scaled))


def activated(values, gain):
    mean = jnp.mean(values * values, axis=0, keepdims=True)
    return silu_of(values, lax.rsqrt(mean + 1e-06), gain)


def column_of(gains, row):
    count = gains.shape[1]
    same = lax.broadcasted_iota(jnp.int32, (count, count), 0) == lax.broadcasted_iota(
        jnp.int32, (count, count), 1
    )
    turned = lax.dot_general(
        jnp.where(same, 1.0, 0.0).astype(BF16),
        gains,
        (((1,), (1,)), ((), ())),
        preferred_element_type=F32,
    )
    return turned[:, row : row + 1]


def rolled(value, step):
    count = value.shape[1]
    return value if step == 0 else pltpu.roll(value, step % count, 1)


def in_order(c, own, other):
    return jnp.where(c == 0, own, other), jnp.where(c == 0, other, own)


def spread(columns, base, stride, value, width, edged):
    depth, count = value.shape
    lane = lax.broadcasted_iota(jnp.int32, value.shape, 1)
    for j in range(3):
        moved = rolled(value, 1 - j)
        if edged and j == 0:
            moved = jnp.where(lane == 0, 0.0, moved)
        if edged and j == 2:
            moved = jnp.where(lane == count - 1, 0.0, moved)
        at = base + j * stride
        columns[at : at + depth, :] = moved[:, :width].astype(BF16)


def in_turn(count, fill, use, buffers):
    fill(0, buffers[0])

    def pair(k, _):
        for side in range(2):
            step = 2 * k + side
            fill(jnp.minimum(step + 1, count - 1), buffers[1 - side])
            use(step, buffers[side])
        return 0

    lax.fori_loop(0, count // 2, pair, 0)
    if count % 2:
        use(count - 1, buffers[0])


def low_sums(total, r, weights, first, frames, columns):
    outs, depth = weights.shape[3:]
    for i in range(3):
        sums = None
        for t in range(frames):
            left = jnp.concatenate([weights[first + t, i, j] for j in range(3)], axis=1)
            part = jnp.dot(
                left, columns[t * 3 * depth : (t + 1) * 3 * depth, :], preferred_element_type=F32
            )
            sums = part if sums is None else sums + part
        total[r + 2 - i] += sums


def low_cached_body(place, own, other, weights, total, *buffers):
    frames, rows, half, width = own.shape
    depth = 2 * half
    c = place[0]
    total[...] = jnp.zeros_like(total)

    def fill(r, columns):
        for t in range(frames):
            for at, value in enumerate(in_order(c, own[t, r], other[t, r])):
                base = t * 3 * depth + at * half
                spread(columns, base, depth, value.astype(F32), width, True)

    def use(r, columns):
        low_sums(total, r, weights, 0, frames, columns)

    in_turn(rows, fill, use, buffers)


def low_living_body(
    which, place, own, other, gain, other_gain, cached, weights, inner, red, black, total, *buffers
):
    rows, half, width = own.shape
    depth = 2 * half
    c, even = place[0], place[3]
    total[...] = cached[...]
    mine = column_of(gain[...], which)
    theirs = column_of(other_gain[...], which)

    def fill(r, columns):
        a, b = own[r].astype(F32), other[r].astype(F32)
        squares = jnp.sum(a * a, axis=0, keepdims=True) + jnp.sum(b * b, axis=0, keepdims=True)
        scale = lax.rsqrt(squares / depth + 1e-06)
        a, b = in_order(c, silu_of(a, scale, mine), silu_of(b, scale, theirs))
        spread(columns, 0, depth, a, width, True)
        spread(columns, half, depth, b, width, True)

    def use(r, columns):
        low_sums(total, r, weights, weights.shape[0] - 1, 1, columns)

    in_turn(rows, fill, use, buffers)
    inner[...] = total[1 : rows + 1]
    up, down = total[0].astype(BF16), total[rows + 1].astype(BF16)
    red[...] = jnp.where(even == 1, down, up)
    black[...] = jnp.where(even == 1, up, down)


def low_cached(place, own, other, kernel):
    frames, rows, half, width = own.shape
    outs, depth = kernel.shape[3:]
    return call(
        low_cached_body,
        "low_cached",
        (place, own, other, kernel),
        [jax.ShapeDtypeStruct((rows + 2, outs, width), F32)],
        [pltpu.VMEM((frames * 3 * depth, width), BF16)] * 2,
        2 * frames * 9 * outs * depth * rows * width,
    )[0]


def low_living(place, own, other, gain, other_gain, which, cached, kernel):
    rows, half, width = own.shape
    outs, depth = kernel.shape[3:]
    return call(
        functools.partial(low_living_body, which),
        "low_living",
        (place, own, other, gain, other_gain, cached, kernel),
        [
            jax.ShapeDtypeStruct((rows, outs, width), F32),
            jax.ShapeDtypeStruct((outs, width), BF16),
            jax.ShapeDtypeStruct((outs, width), BF16),
        ],
        [pltpu.VMEM((rows + 2, outs, width), F32)]
        + [pltpu.VMEM((3 * depth, width), BF16)] * 2,
        2 * 9 * outs * depth * rows * width,
    )


def one_hot(condition):
    return jnp.where(condition, 1.0, 0.0).astype(BF16)


def line_body(place, kernel_a, kernel_b, kernel_r, packet, lined):
    frames, _, _, share, depth = kernel_a.shape
    last = frames - 1
    long = last * 3 * depth
    for i in range(3):
        rows = slice(i * share, (i + 1) * share)
        for j in range(3):
            for t in range(frames):
                at = (t * 3 + j) * depth
                lined[rows, at : at + depth] = kernel_a[t, i, j].astype(F32)
                at = long + 3 * depth + (j * depth if t == last else (3 + t * 3 + j) * depth)
                lined[rows, at : at + depth] = kernel_b[t, i, j].astype(F32)
            at = 2 * long + 6 * depth + 2 * j * depth
            lined[rows, at : at + 2 * depth] = kernel_r[i, j].astype(F32)
    lanes = packet.shape[1]
    total = 2 * long + 12 * depth
    for view in range(lined.shape[1] // lanes):
        @pl.when(place[4] == view)
        def _():
            stop = min(total, (view + 1) * lanes)
            packet[:, : stop - view * lanes] = lined[:, view * lanes : stop].astype(BF16)


def lined_up(place, kernel_a, kernel_b, kernel_r, lanes, pieces):
    share = kernel_a.shape[3]
    return call(
        line_body,
        "line",
        (place, kernel_a, kernel_b, kernel_r),
        [jax.ShapeDtypeStruct((3 * share, lanes), BF16)],
        [pltpu.VMEM((3 * share, lanes * pieces), F32)],
        2 * 3 * share * lanes,
        grant=63 * MIB,
    )[0]


def edge_body(place, cache_a, cache_b, packet):
    frames, rows, depth, width = cache_a.shape
    c = place[0]
    source = lax.broadcasted_iota(jnp.int32, (width, 128), 0)
    lane = lax.broadcasted_iota(jnp.int32, (width, 128), 1)
    start = jnp.where(c == 0, width - 2, 0)
    near = jnp.where(c == 0, width - 1, 0)
    sums = jnp.zeros((depth, 128), F32)
    for t in range(frames):
        for r in range(rows):
            k = lane - 2 * (t * rows + r)
            pick = one_hot((k >= 0) & (k < 2) & (source == start + k))
            sums += jnp.dot(cache_a[t, r], pick, preferred_element_type=F32)
            at = 2 * frames * rows + t * rows + r
            pick = one_hot((lane == at) & (source == near))
            sums += jnp.dot(cache_b[t, r], pick, preferred_element_type=F32)
    packet[...] = sums.astype(BF16)


def edges_of(place, cache_a, cache_b):
    frames, rows, depth, _ = cache_a.shape
    return call(
        edge_body,
        "edges",
        (place, cache_a, cache_b),
        [jax.ShapeDtypeStruct((depth, 128), BF16)],
        [],
        4 * frames * rows * depth * 256 * 128,
    )[0]


def close_body(place, latent, inner, red, black, kept, kept_edge, sent):
    rows, outs, width = latent.shape
    span = width // 2
    c, even = place[0], place[3]
    source = lax.broadcasted_iota(jnp.int32, (width, 128), 0)
    lane = lax.broadcasted_iota(jnp.int32, (width, 128), 1)
    mine = jnp.where(c == 0, span, span - 2)
    theirs = jnp.where(c == 0, span - 2, span)
    edge_mine = jnp.zeros((outs, 128), F32)
    edge_theirs = jnp.zeros((outs, 128), F32)
    for r in range(rows):
        value = latent[r].astype(F32) + inner[r]
        if r == 0:
            value += jnp.where(even == 1, black[...], red[...]).astype(F32)
        if r == rows - 1:
            value += jnp.where(even == 1, red[...], black[...]).astype(F32)
        value = value.astype(BF16)
        left, right = value[:, :span], value[:, span:]
        kept[r] = jnp.where(c == 0, left, right)
        sent[r] = jnp.where(c == 0, right, left)
        k = lane - 2 * (c * rows + r)
        inside = (k >= 0) & (k < 2)
        edge_mine += jnp.dot(
            value, one_hot(inside & (source == mine + k)), preferred_element_type=F32
        )
        edge_theirs += jnp.dot(
            value, one_hot(inside & (source == theirs + k)), preferred_element_type=F32
        )
    kept_edge[...] = edge_mine.astype(BF16)
    sent[rows] = edge_theirs.astype(BF16)


def close(place, latent, inner, red, black):
    rows, outs, width = latent.shape
    span = width // 2
    return call(
        close_body,
        "close",
        (place, latent, inner, red, black),
        [
            jax.ShapeDtypeStruct((rows, outs, span), BF16),
            jax.ShapeDtypeStruct((outs, 128), BF16),
            jax.ShapeDtypeStruct((rows + 1, outs, span), BF16),
        ],
        [],
        4 * rows * outs * width * 128,
    )


def high_sums(total, first, held, columns, width, share):
    outs = total.shape[1]
    group = min(2, outs // share)
    for s in range(0, outs // share, group):
        rows = slice(3 * s * share, 3 * (s + group) * share)
        part = jnp.dot(held[rows], columns[:, :width], preferred_element_type=F32)
        for g in range(group):
            for i in range(3):
                at = 3 * g + i
                total[first + 2 - i, (s + g) * share : (s + g + 1) * share, :] += part[
                    at * share : (at + 1) * share
                ]


def fetches(weights, first, held, sems):
    height, count = held.shape
    lanes = weights.shape[1]
    copies, at = [], 0
    while at < count:
        piece, start = divmod(first + at, lanes)
        size = min(lanes - start, count - at)
        copies.append(
            pltpu.make_async_copy(
                weights.at[piece * height : (piece + 1) * height, start : start + size],
                held.at[:, at : at + size],
                sems.at[len(copies)],
            )
        )
        at += size
    return copies


def every(copies, act):
    for copy in copies:
        getattr(copy, act)()


def kept_lanes(c, width, shape):
    lane = lax.broadcasted_iota(jnp.int32, shape, 1)
    count = shape[1]
    middle = (width + count) // 2
    return (lane < jnp.where(c == 0, middle, width)) | (lane >= jnp.where(c == 0, count, middle))


def high_cached_body(
    share, place, own_a, own_b, edge, weights, sums_a, sums_b, red, black, total_a, total_b,
    columns_a0, columns_a1, columns_b0, columns_b1, held_a, held_b, sems_a, sems_b,
):
    frames, rows, depth, width = own_a.shape
    count = total_a.shape[2]
    c, even = place[0], place[3]
    long = frames * 3 * depth
    copies = fetches(weights, 0, held_a, sems_a) + fetches(weights, long + 6 * depth, held_b, sems_b)
    every(copies, "start")
    total_a[...] = jnp.zeros_like(total_a)
    total_b[...] = jnp.zeros_like(total_b)
    lane = lax.broadcasted_iota(jnp.int32, (depth, 128), 1)

    def fill(r, columns):
        for t in range(frames):
            at = t * rows + r
            first = jnp.where(c == 0, 0, 126)
            moved = pltpu.roll(edge[...].astype(F32), (first - 2 * at + 256) % 128, 1)
            beside = jnp.where((lane >= first) & (lane < first + 2), moved, 0.0)
            value = jnp.concatenate([own_a[t, r].astype(F32), beside], axis=1)
            spread(columns[0], t * 3 * depth, depth, value, count, False)
            at += 2 * frames * rows
            first = jnp.where(c == 0, 0, 127)
            moved = pltpu.roll(edge[...].astype(F32), (first - at + 256) % 128, 1)
            beside = jnp.where(lane == first, moved, 0.0)
            value = jnp.concatenate([own_b[t, r].astype(F32), beside], axis=1)
            spread(columns[1], t * 3 * depth, depth, value, width, False)

    def use(r, columns):
        high_sums(total_a, r, held_a, columns[0], count, share)
        high_sums(total_b, r, held_b, columns[1], width, share)

    every(copies, "wait")
    in_turn(rows, fill, use, ((columns_a0, columns_b0), (columns_a1, columns_b1)))
    sums_a[...] = total_a[...]
    sums_b[...] = total_b[1 : rows + 1]
    spot = 0
    for source, top, bottom in (
        (total_a, 0, rows), (total_a, 1, rows + 1), (total_b, 0, rows + 1)
    ):
        for start in range(0, source.shape[2], 128):
            lanes = slice(start, start + 128)
            up, down = source[top, :, lanes].astype(BF16), source[bottom, :, lanes].astype(BF16)
            red[spot] = jnp.where(even == 1, down, up)
            black[spot] = jnp.where(even == 1, up, down)
            spot += 1


def high_cached(place, own_a, own_b, edge, weights, share):
    frames, rows, depth, width = own_a.shape
    count = width + 128
    blocks = (2 * count + width) // 128
    return call(
        functools.partial(high_cached_body, share),
        "high_cached",
        (place, own_a, own_b, edge),
        [
            jax.ShapeDtypeStruct((rows + 2, depth, count), F32),
            jax.ShapeDtypeStruct((rows, depth, width), F32),
            jax.ShapeDtypeStruct((blocks, depth, 128), BF16),
            jax.ShapeDtypeStruct((blocks, depth, 128), BF16),
        ],
        [
            pltpu.VMEM((rows + 2, depth, count), F32),
            pltpu.VMEM((rows + 2, depth, width), F32),
        ]
        + [pltpu.VMEM((frames * 3 * depth, count), BF16)] * 2
        + [pltpu.VMEM((frames * 3 * depth, width), BF16)] * 2
        + [pltpu.VMEM((3 * depth, frames * 3 * depth), BF16)] * 2
        + [pltpu.SemaphoreType.DMA((8,))] * 2,
        2 * frames * 9 * depth * depth * rows * (width + count),
        (weights,),
    )


def resample_body(
    share, place, one, above, below, weights, resampled, wide, total, columns_0, columns_1, held,
    sems,
):
    blocks, half, span = one.shape
    rows = (blocks - 1) // 2
    _, outs, count = resampled.shape
    high_rows, width = 2 * rows, 2 * span
    c, first, last = place[0], place[1], place[2]
    depth = 2 * half
    copies = fetches(weights, 18 * outs, held, sems)
    every(copies, "start")

    lane = lax.broadcasted_iota(jnp.int32, (span + 128, count), 1)
    source = lax.broadcasted_iota(jnp.int32, (span + 128, count), 0)
    column = jnp.where((c == 1) & (lane >= (width + count) // 2), lane - count, lane) + c * width
    low = column >> 1
    inside = low - c * span
    k = low - jnp.where(c == 0, span, span - 2)
    own_lane = (source == inside) & (inside < span)
    for g in range(2):
        for r in range(rows):
            edge_lane = (source == span + 2 * (g * rows + r) + k) & (k >= 0) & (k < 2)
            edge_lane = edge_lane & ((inside < 0) | (inside >= span))
            spot = kept_lanes(c, width, column.shape) & (own_lane | edge_lane)
            wide[g * rows + r] = one_hot(spot)

    total[...] = jnp.zeros_like(total)

    def fill_low(tile, r, columns):
        for at, value in enumerate(in_order(c, tile[r], tile[rows + r])):
            value = jnp.concatenate([value, tile[2 * rows]], axis=1)
            value = jnp.dot(value, wide[at * rows + r], preferred_element_type=F32)
            spread(columns, at * half, depth, value, count, False)

    def use_low(m, columns):
        group = min(2, outs // share)
        for s in range(0, outs // share, group):
            picked = slice(3 * s * share, 3 * (s + group) * share)
            part = jnp.dot(held[picked], columns[...], preferred_element_type=F32)
            for g in range(group):
                at = slice((s + g) * share, (s + g + 1) * share)
                p0, p1, p2 = (
                    part[(3 * g + i) * share : (3 * g + i + 1) * share] for i in range(3)
                )
                total[2 * m, at, :] += p2
                total[2 * m + 1, at, :] += p1 + p2
                total[2 * m + 2, at, :] += p0 + p1
                total[2 * m + 3, at, :] += p0

    buffers = (columns_0, columns_1)
    steps = [(one, rows)] + [(above, 0)] + [(below, 2 * rows)]
    steps = [(tile, r, at + r) for tile, at in steps for r in range(rows)]
    fill_low(steps[0][0], steps[0][1], buffers[0])
    every(copies, "wait")
    for k, (tile, r, at) in enumerate(steps):
        if k + 1 < len(steps):
            fill_low(steps[k + 1][0], steps[k + 1][1], buffers[(k + 1) % 2])
        use_low(at, buffers[k % 2])

    keep = kept_lanes(c, width, (outs, count))
    for h in range(high_rows + 4):
        value = jnp.where(keep, total[h + 2 * rows - 1], 0.0).astype(BF16)
        if h < 2 or h >= high_rows + 2:
            outside = (first if h < 2 else last) == 1
            value = jnp.where(outside, jnp.zeros_like(value), value)
        resampled[h] = value


def resample(place, one, above, below, weights, outs, share):
    blocks, half, span = one.shape
    rows = (blocks - 1) // 2
    count = 2 * span + 128
    depth = 2 * half
    return call(
        functools.partial(resample_body, share),
        "resample",
        (place, one, above, below),
        [jax.ShapeDtypeStruct((2 * rows + 4, outs, count), BF16)],
        [
            pltpu.VMEM((2 * rows, span + 128, count), BF16),
            pltpu.VMEM((6 * rows + 2, outs, count), F32),
        ]
        + [pltpu.VMEM((3 * depth, count), BF16)] * 2
        + [pltpu.VMEM((3 * outs, 3 * depth), BF16), pltpu.SemaphoreType.DMA((8,))],
        2 * 9 * outs * depth * 2 * rows * count,
        (weights,),
    )[0]


def high_living_body(
    share, place, resampled, gain_a, gain_b, sums_a, sums_b, red, black, weights, decoded,
    total_a, total_b, columns_0, columns_1, held_a, held_b, sems_a, sems_b,
):
    high_rows, outs, width = decoded.shape
    count = sums_a.shape[2]
    c, first, last, even = place[0], place[1], place[2], place[3]
    long = 6 * outs
    padded = columns_0.shape[0]
    copies_a = fetches(weights, long, held_a, sems_a)
    copies_b = fetches(weights, 2 * long - padded, held_b, sems_b)
    every(copies_a + copies_b, "start")
    keep = kept_lanes(c, width, (outs, count))

    total_a[...] = jnp.zeros_like(total_a)
    total_a[2 : high_rows + 4] = sums_a[...]
    total_b[...] = jnp.zeros_like(total_b)
    total_b[2 : high_rows + 2] = sums_b[...]
    spot = 0
    for target, top, bottom in (
        (total_a, 2, high_rows + 2), (total_a, 3, high_rows + 3), (total_b, 2, high_rows + 1)
    ):
        for start in range(0, target.shape[2], 128):
            lanes = slice(start, start + 128)
            a, b = red[spot].astype(F32), black[spot].astype(F32)
            target[top, :, lanes] += jnp.where(even == 1, b, a)
            target[bottom, :, lanes] += jnp.where(even == 1, a, b)
            spot += 1

    buffers = (columns_0, columns_1)
    pad = columns_0.shape[0] - 3 * outs
    for columns in buffers:
        columns[3 * outs :, :] = jnp.zeros((pad, count), BF16)
    left_a, left_b = column_of(gain_a[...], 0), column_of(gain_b[...], 0)

    def fill_a(h, columns):
        value = resampled[h].astype(F32)
        spread(columns, 0, outs, activated(value, left_a), count, False)

    def use_a(h, columns):
        high_sums(total_a, h, held_a, columns, count, share)

    every(copies_a, "wait")
    in_turn(high_rows + 4, fill_a, use_a, buffers)
    every(copies_b, "wait")
    for columns in buffers:
        columns[:pad, :] = jnp.zeros((pad, count), BF16)

    def fill_b(h, columns):
        outside = ((first == 1) & (h < 1)) | ((last == 1) & (h >= high_rows + 1))
        value = jnp.where(keep, total_a[h + 2], 0.0).astype(BF16)
        value = jnp.where(outside, jnp.zeros_like(value), value)
        spread(columns, pad, outs, activated(value.astype(F32), left_b), count, False)

    def use_b(h, columns):
        high_sums(total_b, h, held_b, columns, width, share)

    in_turn(high_rows + 2, fill_b, use_b, buffers)
    for h in range(high_rows):
        decoded[h] = (total_b[h + 2] + resampled[h + 2, :, :width].astype(F32)).astype(BF16)


def high_living(place, resampled, gain_a, gain_b, sums_a, sums_b, red, black, weights, share):
    high_rows, outs, width = sums_b.shape
    count = sums_a.shape[2]
    padded = -(-3 * outs // 128) * 128
    return call(
        functools.partial(high_living_body, share),
        "high_living",
        (place, resampled, gain_a, gain_b, sums_a, sums_b, red, black),
        [jax.ShapeDtypeStruct((high_rows, outs, width), BF16)],
        [
            pltpu.VMEM((high_rows + 6, outs, count), F32),
            pltpu.VMEM((high_rows + 4, outs, width), F32),
        ]
        + [pltpu.VMEM((padded, count), BF16)] * 2
        + [pltpu.VMEM((3 * outs, padded), BF16)] * 2
        + [pltpu.SemaphoreType.DMA((8,))] * 2,
        2 * 27 * outs * outs * high_rows * width,
        (weights,),
    )[0]


def body(
    latent,
    cache_low_a,
    cache_low_b,
    gain_low_a,
    gain_low_b,
    kernel_low_a,
    kernel_low_b,
    resample_kernel,
    gain_high_a,
    gain_high_b,
    kernel_high_a,
    kernel_high_b,
    cache_high_a,
    cache_high_b,
):
    c = lax.axis_index("chan")
    r = lax.axis_index("rows")
    row_count = lax.axis_size("rows")
    swap = [(0, 1), (1, 0)]

    def other_half(value):
        return lax.ppermute(value, "chan", swap)

    reds = [(i, i ^ 1) for i in range(row_count) if i ^ 1 < row_count]
    blacks = [(i, i + 1 if i % 2 else i - 1) for i in range(1, row_count - 1 + row_count % 2)]

    def by_red(value):
        return lax.ppermute(value, "rows", reds)

    def by_black(value):
        return lax.ppermute(value, "rows", blacks)

    even = r % 2 == 0
    view, pieces = lax.axis_index("views"), lax.axis_size("views")
    place = jnp.stack([c, r == 0, r == row_count - 1, even, view]).astype(jnp.int32)

    share, outs = kernel_high_a.shape[3:]
    height = 3 * share
    count = 18 * outs + 3 * resample_kernel.shape[3]
    lanes = -(-count // (128 * pieces)) * 128
    if share % 8:

        def flat(kernel):
            return jnp.transpose(kernel, (1, 3, 0, 2, 4)).reshape(height, -1)

        flat_a, flat_b = flat(kernel_high_a), flat(kernel_high_b)
        lined = [flat_a, flat_b[:, 6 * outs :], flat_b[:, : 6 * outs], flat(resample_kernel[None])]
        lined = jnp.pad(jnp.concatenate(lined, axis=1), ((0, 0), (0, lanes * pieces - count)))
        mine = lax.dynamic_slice_in_dim(lined, view * lanes, lanes, 1)
        weights = lax.all_gather(mine, ("views", "rows"), axis=0, tiled=True)
        weights = weights.reshape(pieces, row_count, 3, share, lanes).transpose(0, 2, 1, 3, 4)
        weights = weights.reshape(-1, lanes)
        share = outs
    else:
        with jax.named_scope("prep"):
            mine = lined_up(
                place, kernel_high_a, kernel_high_b, resample_kernel, lanes, pieces
            )
        weights = lax.all_gather(mine, ("views", "rows"), axis=0, tiled=True)

    rows, half, low_width = latent.shape
    gains = jnp.pad(jnp.stack([gain_low_a, gain_low_b]), ((0, 14), (0, 0)))
    sent = jnp.pad(gains, ((0, 0), (0, low_width - half)))
    sent = jnp.concatenate([latent.reshape(rows * half, low_width), sent])
    with jax.named_scope("e0"):
        got = other_half(sent)
    other_latent = got[: rows * half].reshape(latent.shape)
    other_gains = got[rows * half :, :half]
    with jax.named_scope("e0a"):
        other_cache_a = other_half(cache_low_a)
    with jax.named_scope("e0b"):
        other_cache_b = other_half(cache_low_b)
    with jax.named_scope("e0s"):
        edge = other_half(edges_of(place, cache_high_a, cache_high_b))

    def low_conv(inputs, other, cached, which, kernel):
        inner, red, black = low_living(
            place, inputs, other, gains, other_gains, which, cached, kernel
        )
        return inner, by_red(red), by_black(black)

    cached_a = low_cached(place, cache_low_a, other_cache_a, kernel_low_a)
    cached_b = low_cached(place, cache_low_b, other_cache_b, kernel_low_b)
    inner, red, black = low_conv(latent, other_latent, cached_a, 0, kernel_low_a)
    top = jnp.where(even, black, red).astype(F32)
    bottom = jnp.where(even, red, black).astype(F32)
    middle_low = jnp.concatenate(
        [inner[:1] + top, inner[1:-1], inner[-1:] + bottom]
    ).astype(BF16)
    inner, red, black = low_conv(middle_low, other_half(middle_low), cached_b, 1, kernel_low_b)
    kept, kept_edge, sent = close(place, latent, inner, red, black)
    got = other_half(sent)
    one = jnp.concatenate([kept, got[:rows], (kept_edge + got[rows])[None]])
    from_red, from_black = by_red(one), by_black(one)
    above = jnp.where(even, from_black, from_red)
    below = jnp.where(even, from_red, from_black)

    sums_a, sums_b, red, black = high_cached(
        place, cache_high_a, cache_high_b, edge, weights, share
    )
    with jax.named_scope("sumred"):
        red = by_red(red)
    with jax.named_scope("sumblack"):
        black = by_black(black)
    with jax.named_scope("resampled"):
        resampled = resample(place, one, above, below, weights, outs, share)
    return high_living(
        place,
        resampled,
        jnp.pad(gain_high_a[None], ((0, 15), (0, 0))),
        jnp.pad(gain_high_b[None], ((0, 15), (0, 0))),
        sums_a,
        sums_b,
        red,
        black,
        weights,
        share,
    )


def solution(mesh):
    placed = (
        P(("views", "rows"), "chan", None),
        P(None, ("views", "rows"), "chan", None),
        P(None, ("views", "rows"), "chan", None),
        P("chan"),
        P("chan"),
        P(None, None, None, "chan", None),
        P(None, None, None, "chan", None),
        P(None, None, "rows", None),
        P(),
        P(),
        P(None, None, None, "rows", None),
        P(None, None, None, "rows", None),
        P(None, ("views", "rows"), None, "chan"),
        P(None, ("views", "rows"), None, "chan"),
    )
    return jax.shard_map(
        body,
        mesh=mesh,
        in_specs=placed,
        out_specs=P(("views", "rows"), None, "chan"),
        check_vma=False,
    )
```
